32 devices in a mesh: scen: 2 (over x), gx: 16 (over z, y, core).
Axes of the slice: x: 2, y: 2, z: 4, core: 2. Of those that a mesh axis runs over, the one named last changes fastest.
Arguments:
- populations: float32 [54, 16, 4, 8, 256], P('scen', 'gx'), parts along dimension 0, may hold values from 0.15 to 2
- cell_kind: int32 [16, 4, 8, 512], P('gx', None, None, 'scen'), parts along dimension 3, may hold values from 0 to 4, as said below
- profile: int32 [16, 4, 8, 512], P('gx', None, None, 'scen'), parts along dimension 3, may hold values from 0 to 7
- vent_table: float32 [16, 3], P('scen'), parts along dimension 0, may hold values from -0.08 to 0.08
- rates: float32 [27], replicated, may hold values from 1 to 1.9
Outputs:
- advanced: float32 [54, 16, 4, 8, 256], P('scen', 'gx'), parts along dimension 0
The draws below stay inside these ranges and needn't reach their ends.
There are 2 independent parts, one for each index of `scen`. The reference program is written for one: setup_inputs(seed, part) draws one part's arguments, and reference() takes and returns one part's arrays. A program takes and returns all parts, laid end to end along the dimension named above; an argument that names none is the same for every part. Nothing has to cross between parts.
Inputs may be any that keep to these rules, and one draw needn't show every extreme that they name: `cell_kind`: 0 fluid, 1 wall, 2 vent, 3 inflow, 4 outflow.
All inputs are finite; a program needn't handle non-finite values.
Results may differ from the reference program's by a relative error of at most 0.0003.
Values sent between devices are 32-bit elements; how exact they have to be, the bound alone decides.
No kernel may reach another device: no remote copies, remote signals or barrier semaphores. Data moves between devices by JAX's collectives and lax.ppermute only.
A program may use at most 64 MiB of HBM per device.

```python
import jax
import jax.numpy as jnp
import numpy as np
from jax import lax

PY = 8
CX = 4
CY = 8
NZ = 256
STEPS = 3
PROFILES = 8
BLOCKS = 16


def draw_populations(key, part):
    first_key, second_key, third_key = jax.random.split(key, 3)
    velocity = jnp.clip(jax.random.normal(first_key, (3, BLOCKS, CX, CY, NZ), jnp.float32) * 0.03, -0.05, 0.05)
    density = 1.0 + jax.random.uniform(third_key, (BLOCKS, CX, CY, NZ), jnp.float32, -0.1, 0.1)
    deviation = jnp.clip(jax.random.normal(second_key, (27, BLOCKS, CX, CY, NZ), jnp.float32) * 0.12, -0.3, 0.3)
    columns = []
    for k in range(27):
        step_x = float(k // 9 - 1)
        step_y = float(k // 3 % 3 - 1)
        step_z = float(k % 3 - 1)
        projected = step_x * velocity[0] + step_y * velocity[1] + step_z * velocity[2]
        columns.append(density * (1.0 + 3.0 * projected))
    return jnp.stack(columns) + deviation


def draw_cell_kind(key, part):
    ticket = jax.random.randint(key, (BLOCKS, CX, CY, NZ), 0, 100)
    return jnp.where(ticket < 70, 0, jnp.where(ticket < 80, 1, jnp.where(ticket < 88, 2, jnp.where(ticket < 94, 3, 4)))).astype(jnp.int32)


def with_ends(drawn, own_key, least, high):
    spot = [jax.random.randint(jax.random.fold_in(own_key, axis), (), 0, length) for axis, length in enumerate(drawn.shape)]
    longest = drawn.shape.index(max(drawn.shape))
    neighbour = spot[:longest] + [(spot[longest] + 1) % drawn.shape[longest]] + spot[longest + 1:]
    return drawn.at[tuple(spot)].set(least).at[tuple(neighbour)].set(high)


def setup_inputs(seed: int = 0, part: int = 0) -> dict:
    key_of = jax.random.split(jax.random.key(seed), 6)
    part_keys = jax.random.split(jax.random.fold_in(key_of[5], part), 6)
    return {
        "populations": draw_populations(jax.random.fold_in(jax.random.fold_in(key_of[5], part), 71), part),
        "cell_kind": draw_cell_kind(jax.random.fold_in(jax.random.fold_in(key_of[5], part), 71), part),
        "profile": with_ends(jax.random.randint(part_keys[2], (BLOCKS, CX, CY, NZ), 0, PROFILES), jax.random.fold_in(part_keys[2], 1), 0, PROFILES - 1).astype(jnp.int32),
        "vent_table": jnp.clip(jax.random.uniform(part_keys[3], (PROFILES, 3), jnp.float32, -0.08, 0.08), -0.08, 0.08),
        "rates": jnp.clip(jax.random.uniform(key_of[4], (27,), jnp.float32, 1.0, 1.9), 1.0, 1.9),
    }


def lattice_tables():
    speeds = np.array([[a - 1.0, b - 1.0, d - 1.0] for a in range(3) for b in range(3) for d in range(3)])
    single = np.array([1.0 / 6.0, 2.0 / 3.0, 1.0 / 6.0])
    weights = np.kron(np.kron(single, single), single)
    powers = np.array([[1.0, 1.0, 1.0], [-1.0, 0.0, 1.0], [1.0, 0.0, 1.0]])
    undo = np.array([[0.0, -0.5, 0.5], [1.0, 0.0, -1.0], [0.0, 0.5, 0.5]])
    moments = np.kron(np.kron(powers, powers), powers)
    inverse = np.kron(np.kron(undo, undo), undo)
    return speeds, weights, moments, inverse


def relax_matrix(rates):
    speeds, weights, moments, inverse = lattice_tables()
    left_part = jnp.asarray(inverse / weights[:, None], jnp.float32) * rates[None, :]
    right_part = jnp.asarray(moments * weights[None, :], jnp.float32)
    return jnp.dot(left_part, right_part, precision=lax.Precision.HIGHEST)


def equilibrium(density, velocity):
    speeds = lattice_tables()[0]
    square = velocity[0] * velocity[0] + velocity[1] * velocity[1] + velocity[2] * velocity[2]
    columns = []
    for k in range(27):
        projected = float(speeds[k, 0]) * velocity[0] + float(speeds[k, 1]) * velocity[1] + float(speeds[k, 2]) * velocity[2]
        columns.append(density * (1.0 + 3.0 * projected + 4.5 * projected * projected - 1.5 * square))
    return jnp.stack(columns)


def macroscopic(scaled):
    speeds, weights, moments, inverse = lattice_tables()
    weight_vec = jnp.asarray(weights, jnp.float32)
    moment_rows = jnp.asarray((weights[:, None] * speeds).T, jnp.float32)
    density = jnp.tensordot(weight_vec, scaled, axes=1, precision=lax.Precision.HIGHEST)
    momentum = jnp.tensordot(moment_rows, scaled, axes=1, precision=lax.Precision.HIGHEST)
    return density, momentum / density[None]


def collide(scaled, matrix):
    density, velocity = macroscopic(scaled)
    layout = scaled.shape
    flattened = (scaled - equilibrium(density, velocity)).reshape(27, -1)
    return scaled - jnp.dot(matrix, flattened, precision=lax.Precision.HIGHEST).reshape(layout)


def profile_velocity(profile, vent_table):
    matches = (profile[None] == jnp.arange(vent_table.shape[0], dtype=jnp.int32)[:, None, None, None]).astype(vent_table.dtype)
    return jnp.tensordot(vent_table.T, matches, axes=1, precision=lax.Precision.HIGHEST)


def finish_pull(collided, shifted_x, types_pad, wall_pad, k):
    speeds = lattice_tables()[0]
    step_x, step_y, step_z = int(speeds[k, 0]), int(speeds[k, 1]), int(speeds[k, 2])
    width_x, width_y, width_z = collided.shape[1], collided.shape[2], collided.shape[3]
    padded = jnp.pad(shifted_x, ((0, 0), (1, 1), (1, 1)))
    source = padded[:, 1 - step_y:1 - step_y + width_y, 1 - step_z:1 - step_z + width_z]
    types_src = types_pad[1 - step_x:1 - step_x + width_x, 1 - step_y:1 - step_y + width_y, 1 - step_z:1 - step_z + width_z]
    wall_src = wall_pad[:, 1 - step_x:1 - step_x + width_x, 1 - step_y:1 - step_y + width_y, 1 - step_z:1 - step_z + width_z]
    projected = float(step_x) * wall_src[0] + float(step_y) * wall_src[1] + float(step_z) * wall_src[2]
    bounce = collided[26 - k] + jnp.where(types_src == 2, 6.0 * projected, 0.0)
    open_cell = (types_src == 0) | (types_src >= 3)
    return jnp.where(open_cell, source, bounce)


def apply_cells(passed, cell_types, cell_speed):
    density, velocity = macroscopic(passed)
    unity = jnp.ones_like(density)
    forced_in = equilibrium(unity, cell_speed)
    forced_out = equilibrium(unity, velocity)
    result = jnp.where(cell_types == 0, passed, 1.0)
    result = jnp.where(cell_types == 3, forced_in, result)
    return jnp.where(cell_types == 4, forced_out, result)


def to_room(blocked):
    blocked = jnp.roll(blocked, PY // 2, axis=blocked.ndim - 4)
    lead = blocked.shape[:-4]
    count, depth, rows, cells = blocked.shape[-4:]
    split = blocked.reshape(lead + (count // PY, PY, depth, rows, cells))
    split = jnp.swapaxes(split, -4, -3)
    return split.reshape(lead + ((count // PY) * depth, PY * rows, cells))


def to_blocks(room, depth, rows):
    lead = room.shape[:-3]
    cells = room.shape[-1]
    split = room.reshape(lead + (room.shape[-3] // depth, depth, PY, rows, cells))
    split = jnp.swapaxes(split, -4, -3)
    blocked = split.reshape(lead + ((room.shape[-3] // depth) * PY, depth, rows, cells))
    return jnp.roll(blocked, -(PY // 2), axis=blocked.ndim - 4)


def reference(populations, cell_kind, profile, vent_table, rates):
    depth, rows = populations.shape[2], populations.shape[3]
    speeds = lattice_tables()[0]
    matrix = relax_matrix(rates)
    room_kind = to_room(cell_kind)
    room_profile = to_room(profile)
    types_pad = jnp.pad(jnp.pad(room_kind, ((1, 1), (0, 0), (0, 0)), mode="wrap"), ((0, 0), (1, 1), (1, 1)), constant_values=1)
    profile_pad = jnp.pad(jnp.pad(room_profile, ((1, 1), (0, 0), (0, 0)), mode="wrap"), ((0, 0), (1, 1), (1, 1)))
    wall_pad = profile_velocity(profile_pad, vent_table)
    cell_speed = wall_pad[:, 1:-1, 1:-1, 1:-1]
    scaled = to_room(populations)
    for iteration in range(STEPS):
        collided = collide(scaled, matrix)
        pulled = []
        for k in range(27):
            shifted_x = jnp.roll(collided[k], int(speeds[k, 0]), axis=0)
            pulled.append(finish_pull(collided, shifted_x, types_pad, wall_pad, k))
        scaled = apply_cells(jnp.stack(pulled), room_kind, cell_speed)
    return to_blocks(scaled, depth, rows)
```

```python
import functools

import jax
import jax.numpy as jnp
import numpy as np
from jax import lax
from jax.experimental import pallas as pl
from jax.experimental.pallas import tpu as pltpu
from jax.sharding import PartitionSpec as P

PY = 8
STEPS = 3
LANES = 128
OPEN = 1e30
CONSERVED = (0, 9, 3, 1)


def direction(k):
    return k // 9 - 1, k // 3 % 3 - 1, k % 3 - 1


def equilibrium_moments():
    speeds = np.array([direction(k) for k in range(27)], float)
    single = np.array([1.0 / 6.0, 2.0 / 3.0, 1.0 / 6.0])
    weights = np.kron(np.kron(single, single), single)
    powers = np.array([[1.0, 1.0, 1.0], [-1.0, 0.0, 1.0], [1.0, 0.0, 1.0]])
    moments = np.kron(np.kron(powers, powers), powers)
    basis = [np.ones(27)]
    basis += [3.0 * speeds[:, i] for i in range(3)]
    basis += [4.5 * speeds[:, i] ** 2 - 1.5 for i in range(3)]
    basis += [9.0 * speeds[:, i] * speeds[:, j] for i, j in ((0, 1), (0, 2), (1, 2))]
    return 27.0 * moments @ (weights[:, None] * np.stack(basis, 1))


TABLE = equilibrium_moments()


def along_axes(values, change):
    for stride in (9, 3, 1):
        out = list(values)
        for k in range(27):
            if k // stride % 3 == 0:
                trio = (values[k], values[k + stride], values[k + 2 * stride])
                out[k], out[k + stride], out[k + 2 * stride] = change(*trio)
        values = out
    return values


def to_moment(low, mid, high):
    total = low + high
    return total + 4.0 * mid, high - low, total


def from_moment(zeroth, first, second):
    return second - first, 0.5 * (zeroth - second), first + second


def equilibrium_terms(density, velocity):
    ux, uy, uz = velocity
    jx, jy, jz = density * ux, density * uy, density * uz
    terms = (density, jx, jy, jz, jx * ux, jy * uy, jz * uz, jx * uy, jx * uz, jy * uz)
    result = []
    for k in range(27):
        value = None
        for t in range(10):
            coefficient = float(TABLE[k, t])
            if abs(coefficient) > 1e-9:
                piece = terms[t] if abs(coefficient - 1.0) < 1e-9 else coefficient * terms[t]
                value = piece if value is None else value + piece
        result.append(jnp.zeros_like(density) if value is None else value)
    return result


def density_velocity(raw):
    inverse = 1.0 / raw[0]
    return raw[0] * (1.0 / 216.0), (raw[9] * inverse, raw[3] * inverse, raw[1] * inverse)


def vent_velocity(profile, table_ref):
    parts = [jnp.zeros(profile.shape, jnp.float32) for _ in range(3)]
    for p in range(table_ref.shape[0]):
        match = profile == p
        parts = [jnp.where(match, table_ref[p, c], parts[c]) for c in range(3)]
    return parts


def relaxed(raw, equal, rates_ref):
    result = []
    for k in range(27):
        if k in CONSERVED:
            result.append(0.125 * raw[k])
        else:
            rate = rates_ref[k]
            result.append(rate * equal[k] + ((1.0 - rate) * 0.125) * raw[k])
    return result


def tiles(depth, cells, body):
    def plane(x, carry):
        for start in range(0, cells, LANES):
            body(x, slice(start, start + LANES))
        return carry

    lax.fori_loop(0, depth, plane, 0)


def pack(collided, sends, cell_refs):
    send_x, send_up, send_down, corner_up, corner_down = sends
    depth, rows = collided.shape[1], collided.shape[2]
    for side, a, x in ((0, 1, depth - 1), (1, -1, 0)):
        for i in range(9):
            send_x[side, i] = collided[9 * (a + 1) + i, x]
        for i, ref in enumerate(cell_refs):
            send_x[side, 9 + i] = ref[x].astype(jnp.float32)
    for buffer, corner, b, y in ((send_up, corner_up, 1, rows - 1), (send_down, corner_down, -1, 0)):
        for a in (-1, 0, 1):
            for e in (-1, 0, 1):
                k = 9 * (a + 1) + 3 * (b + 1) + e + 1
                first = (3 * (a + 1) + e + 1) * depth
                for x in range(depth):
                    buffer[first + x : first + x + 1, :] = collided[k, x, y : y + 1, :]
        for i, ref in enumerate(cell_refs):
            for x in range(depth):
                at = (9 + i) * depth + x
                buffer[at : at + 1, :] = ref[x, y : y + 1, :].astype(jnp.float32)
        for side, a, x in ((0, 1, depth - 1), (1, -1, 0)):
            for e in (-1, 0, 1):
                k = 9 * (a + 1) + 3 * (b + 1) + e + 1
                corner[side, e + 1 : e + 2, :] = collided[k, x, y : y + 1, :]
            for i, ref in enumerate(cell_refs):
                corner[side, 3 + i : 4 + i, :] = ref[x, y : y + 1, :].astype(jnp.float32)


def first_kernel(populations, kind, profile, rates, collided, *sends):
    depth, cells = populations.shape[1], populations.shape[3]

    def body(x, span):
        raw = along_axes([populations[k, x, :, span] for k in range(27)], to_moment)
        equal = equilibrium_terms(*density_velocity(raw))
        values = along_axes(relaxed(raw, equal, rates), from_moment)
        for k in range(27):
            collided[k, x, :, span] = values[k]

    tiles(depth, cells, body)
    pack(collided, sends, (kind, profile))


def shifted(plane, row, b, e, sublane):
    rows, cells = plane.shape
    if b:
        plane = pltpu.roll(plane, b % rows, 0)
        edge = 0 if b == 1 else rows - 1
        plane = jnp.where(sublane == edge, jnp.broadcast_to(row, plane.shape), plane)
    if e:
        plane = pltpu.roll(plane, e % cells, 1)
    return plane


def cell_fields(kind, profile, table):
    open_cell = (kind == 0) | (kind >= 3)
    vent = kind == 2
    velocity = vent_velocity(profile, table)
    return [jnp.where(open_cell, OPEN, 0.0)] + [jnp.where(vent, 6.0 * v, 0.0) for v in velocity]


def make_fields(halo, kind, profile, table, place, kinds_row, profiles_row, planes, edges):
    recv_x, recv_low, recv_high, corner_low, corner_high = halo
    depth = kind.shape[0]
    for x in range(-1, depth + 1):
        if 0 <= x < depth:
            kinds, profiles = kind[x].astype(jnp.float32), profile[x].astype(jnp.float32)
        else:
            side = 0 if x < 0 else 1
            kinds, profiles = recv_x[side, 9], recv_x[side, 10]
        for c, value in enumerate(cell_fields(kinds, profiles, table)):
            planes[c, x + 1] = value
    row_sides = ((recv_low, corner_low, 0), (recv_high, corner_high, PY - 1))
    for s, (buffer, corner, outer) in enumerate(row_sides):
        for target, i in ((kinds_row, 0), (profiles_row, 1)):
            target[...] = jnp.zeros(target.shape, jnp.float32)
            target[0:1, :] = corner[0, 3 + i : 4 + i, :]
            at = (9 + i) * depth
            for x in range(depth):
                target[x + 1 : x + 2, :] = buffer[at + x : at + x + 1, :]
            target[depth + 1 : depth + 2, :] = corner[1, 3 + i : 4 + i, :]
        kinds = jnp.where(place[0] == outer, 1.0, kinds_row[...])
        for c, value in enumerate(cell_fields(kinds, profiles_row[...], table)):
            edges[s, c] = value


def stream(collided, halo, bounce, passed, fields):
    recv_x, recv_low, recv_high, corner_low, corner_high = halo
    depth, rows, cells = collided.shape[1:]
    sublane = lax.broadcasted_iota(jnp.int32, (rows, cells), 0)
    lane = lax.broadcasted_iota(jnp.int32, (rows, cells), 1)
    for k in range(27):
        a, b, e = direction(k)
        for x in range(depth):
            if k == 13:
                passed[k, x] = collided[k, x]
                continue
            source = x - a
            side = 0 if source < 0 else 1
            inside = 0 <= source < depth
            plane = collided[k, source] if inside else recv_x[side, 3 * (b + 1) + e + 1]
            row = None
            if b:
                buffer, corner = (recv_low, corner_low) if b == 1 else (recv_high, corner_high)
                at = (3 * (a + 1) + e + 1) * depth + source
                row = buffer[at : at + 1, :] if inside else corner[side, e + 1 : e + 2, :]
            if fields is not None:
                planes, edges = fields

                def combine(read):
                    value = read(0)
                    for c, step in enumerate((a, b, e)):
                        if step:
                            value = value + read(c + 1) if step > 0 else value - read(c + 1)
                    return value

                term = combine(lambda c: planes[c, source + 1])
                term_row = None
                if b:
                    s = 0 if b == 1 else 1
                    term_row = combine(lambda c: edges[s, c, source + 1 : source + 2, :])
                term = shifted(term, term_row, b, e, sublane)
                if e:
                    term = jnp.where(lane == (0 if e == 1 else cells - 1), 0.0, term)
                bounce[k, x] = term
            term = bounce[k, x]
            value = shifted(plane, row, b, e, sublane)
            passed[k, x] = jnp.where(term > 0.5 * OPEN, value, collided[26 - k, x] + term)


def chosen(kind, profile, table, velocity):
    vent = vent_velocity(profile, table)
    return [
        jnp.where(kind == 3, vent[c], jnp.where(kind == 4, velocity[c], 0.0)) for c in range(3)
    ]


def collide_cells(passed, kind, profile, table, rates, collided):
    depth, cells = passed.shape[1], passed.shape[3]

    def body(x, span):
        kinds = kind[x, :, span]
        fluid = kinds == 0
        raw = along_axes([passed[k, x, :, span] for k in range(27)], to_moment)
        density, velocity = density_velocity(raw)
        forced = chosen(kinds, profile[x, :, span], table, velocity)
        density = jnp.where(fluid, density, 1.0)
        velocity = [jnp.where(fluid, velocity[c], forced[c]) for c in range(3)]
        equal = equilibrium_terms(density, velocity)
        mixed = relaxed(raw, equal, rates)
        values = [jnp.where(fluid, mixed[k], equal[k]) for k in range(27)]
        values = along_axes(values, from_moment)
        for k in range(27):
            collided[k, x, :, span] = values[k]

    tiles(depth, cells, body)


def finish_cells(passed, kind, profile, table, advanced):
    depth, cells = passed.shape[1], passed.shape[3]

    def body(x, span):
        kinds = kind[x, :, span]
        fluid = kinds == 0
        values = [passed[k, x, :, span] for k in range(27)]
        velocity = density_velocity(along_axes(values, to_moment))[1]
        ux, uy, uz = chosen(kinds, profile[x, :, span], table, velocity)
        base = 1.0 - 1.5 * (ux * ux + uy * uy + uz * uz)
        for k in range(27):
            projected = None
            for step, u in zip(direction(k), (ux, uy, uz)):
                if step:
                    signed = u if step > 0 else -u
                    projected = signed if projected is None else projected + signed
            equal = base if projected is None else base + projected * (3.0 + 4.5 * projected)
            advanced[k, x, :, span] = jnp.where(fluid, values[k], equal)

    tiles(depth, cells, body)


def second_kernel(*refs):
    collided, *halo = refs[:6]
    kind, profile, table, rates, place = refs[6:11]
    out, bounce = refs[11:13]
    sends = refs[13:18]
    passed, kinds_row, profiles_row, planes, edges = refs[18:]
    make_fields(halo, kind, profile, table, place, kinds_row, profiles_row, planes, edges)
    stream(collided, halo, bounce, passed, (planes, edges))
    collide_cells(passed, kind, profile, table, rates, out)
    pack(out, sends, ())


def middle_kernel(*refs):
    collided, *halo = refs[:6]
    bounce, kind, profile, table, rates = refs[6:11]
    out = refs[11]
    sends = refs[12:17]
    passed = refs[17]
    stream(collided, halo, bounce, passed, None)
    collide_cells(passed, kind, profile, table, rates, out)
    pack(out, sends, ())


def last_kernel(*refs):
    collided, *halo = refs[:6]
    bounce, kind, profile, table, advanced, passed = refs[6:]
    stream(collided, halo, bounce, passed, None)
    finish_cells(passed, kind, profile, table, advanced)


def passed_along(value, steps):
    count = lax.axis_size("gx")
    pairs = [(source, (source + steps) % count) for source in range(count)]
    return lax.ppermute(value, "gx", pairs)


def both_sides(value, across):
    if lax.axis_size("gx") == 2 * PY:
        return passed_along(value, PY + across)
    return jnp.stack(
        [passed_along(value[0], PY + across), passed_along(value[1], across - PY)]
    )


def exchange(sends):
    send_x, send_up, send_down, corner_up, corner_down = sends
    return (
        both_sides(send_x, 0),
        passed_along(send_up, 1),
        passed_along(send_down, -1),
        both_sides(corner_up, 1),
        both_sides(corner_down, -1),
    )


def round_up(value, step):
    return -(-value // step) * step


def local(populations, cell_kind, profile, vent_table, rates):
    scaled = populations[:, 0]
    kind, profile = cell_kind[0], profile[0]
    depth, rows, cells = kind.shape
    f32 = jnp.float32
    field = jax.ShapeDtypeStruct(scaled.shape, f32)
    vmem = pl.BlockSpec(memory_space=pltpu.VMEM)
    smem = pl.BlockSpec(memory_space=pltpu.SMEM)
    place = ((lax.axis_index("gx") + PY // 2) % PY).astype(jnp.int32).reshape(1)

    def send_shapes(extra):
        along = jax.ShapeDtypeStruct((round_up((9 + extra) * depth, 8), cells), f32)
        corner = jax.ShapeDtypeStruct((2, 8, cells), f32)
        across = jax.ShapeDtypeStruct((2, 9 + extra, rows, cells), f32)
        return (across, along, along, corner, corner)

    def call(body, specs, outs, scratch, name):
        return pl.pallas_call(
            body,
            in_specs=specs,
            out_specs=jax.tree.map(lambda _: vmem, outs),
            out_shape=outs,
            scratch_shapes=scratch,
            name=name,
        )

    buffer = pltpu.VMEM(scaled.shape, f32)
    edge_rows = round_up(depth + 2, 8)
    collided, *sends = call(
        first_kernel, [vmem] * 3 + [smem], (field,) + send_shapes(2), [], "first"
    )(scaled, kind, profile, rates)
    halo = exchange(sends)
    collided, bounce, *sends = call(
        second_kernel,
        [vmem] * 8 + [smem] * 3,
        (field, field) + send_shapes(0),
        [
            buffer,
            pltpu.VMEM((edge_rows, cells), f32),
            pltpu.VMEM((edge_rows, cells), f32),
            pltpu.VMEM((4, depth + 2, rows, cells), f32),
            pltpu.VMEM((2, 4, edge_rows, cells), f32),
        ],
        "second",
    )(collided, *halo, kind, profile, vent_table, rates, place)
    for _ in range(STEPS - 2):
        halo = exchange(sends)
        collided, *sends = call(
            middle_kernel,
            [vmem] * 9 + [smem] * 2,
            (field,) + send_shapes(0),
            [buffer],
            "middle",
        )(collided, *halo, bounce, kind, profile, vent_table, rates)
    halo = exchange(sends)
    advanced = call(last_kernel, [vmem] * 9 + [smem], field, [buffer], "last")(
        collided, *halo, bounce, kind, profile, vent_table
    )
    return advanced[:, None]


def solution(mesh):
    return jax.shard_map(
        local,
        mesh=mesh,
        in_specs=(
            P("scen", "gx", None, None, None),
            P("gx", None, None, "scen"),
            P("gx", None, None, "scen"),
            P("scen", None),
            P(),
        ),
        out_specs=P("scen", "gx", None, None, None),
        check_vma=False,
    )
```

```python
import functools

import jax
import jax.numpy as jnp
import numpy as np
from jax import lax
from jax.experimental import pallas as pl
from jax.experimental.pallas import tpu as pltpu
from jax.sharding import PartitionSpec as P

PY = 8
STEPS = 3
LANES = 128
OPEN = 1e30
CONSERVED = (0, 9, 3, 1)


def direction(k):
    return k // 9 - 1, k // 3 % 3 - 1, k % 3 - 1


def equilibrium_moments():
    speeds = np.array([direction(k) for k in range(27)], float)
    single = np.array([1.0 / 6.0, 2.0 / 3.0, 1.0 / 6.0])
    weights = np.kron(np.kron(single, single), single)
    powers = np.array([[1.0, 1.0, 1.0], [-1.0, 0.0, 1.0], [1.0, 0.0, 1.0]])
    moments = np.kron(np.kron(powers, powers), powers)
    basis = [np.ones(27)]
    basis += [3.0 * speeds[:, i] for i in range(3)]
    basis += [4.5 * speeds[:, i] ** 2 - 1.5 for i in range(3)]
    basis += [9.0 * speeds[:, i] * speeds[:, j] for i, j in ((0, 1), (0, 2), (1, 2))]
    return 27.0 * moments @ (weights[:, None] * np.stack(basis, 1))


TABLE = equilibrium_moments()


def along_axes(values, change):
    for stride in (9, 3, 1):
        out = list(values)
        for k in range(27):
            if k // stride % 3 == 0:
                trio = (values[k], values[k + stride], values[k + 2 * stride])
                out[k], out[k + stride], out[k + 2 * stride] = change(*trio)
        values = out
    return values


def to_moment(low, mid, high):
    total = low + high
    return total + 4.0 * mid, high - low, total


def from_moment(zeroth, first, second):
    return second - first, 0.5 * (zeroth - second), first + second


def equilibrium_terms(density, velocity):
    ux, uy, uz = velocity
    jx, jy, jz = density * ux, density * uy, density * uz
    terms = (density, jx, jy, jz, jx * ux, jy * uy, jz * uz, jx * uy, jx * uz, jy * uz)
    result = []
    for k in range(27):
        value = None
        for t in range(10):
            coefficient = float(TABLE[k, t])
            if abs(coefficient) > 1e-9:
                piece = terms[t] if abs(coefficient - 1.0) < 1e-9 else coefficient * terms[t]
                value = piece if value is None else value + piece
        result.append(jnp.zeros_like(density) if value is None else value)
    return result


def density_velocity(raw):
    inverse = 1.0 / raw[0]
    return raw[0] * (1.0 / 216.0), (raw[9] * inverse, raw[3] * inverse, raw[1] * inverse)


def vent_velocity(profile, table_ref):
    parts = [jnp.zeros(profile.shape, jnp.float32) for _ in range(3)]
    for p in range(table_ref.shape[0]):
        match = profile == p
        parts = [jnp.where(match, table_ref[p, c], parts[c]) for c in range(3)]
    return parts


def relaxed(raw, equal, rates_ref):
    result = []
    for k in range(27):
        if k in CONSERVED:
            result.append(0.125 * raw[k])
        else:
            rate = rates_ref[k]
            result.append(rate * equal[k] + ((1.0 - rate) * 0.125) * raw[k])
    return result


def tiles(depth, cells, body):
    def plane(x, carry):
        for start in range(0, cells, LANES):
            body(x, slice(start, start + LANES))
        return carry

    lax.fori_loop(0, depth, plane, 0)


class Planes:
    def __init__(self, edge, inner):
        self.edge, self.inner = edge, inner
        self.depth = inner.shape[1] + 2

    def __getitem__(self, index):
        k, x = index[0], index[1]
        rest = tuple(index[2:])
        if x == 0:
            return self.edge[(k, 0) + rest]
        if x == self.depth - 1:
            return self.edge[(k, 1) + rest]
        return self.inner[(k, x - 1) + rest]


def pack_x(edge, send_x, cell_refs):
    for side, a, at in ((0, 1, 1), (1, -1, 0)):
        for i in range(9):
            send_x[side, i] = edge[9 * (a + 1) + i, at]
        for i, ref in enumerate(cell_refs):
            send_x[side, 9 + i] = ref[(ref.shape[0] - 1) * at].astype(jnp.float32)


def pack_y(field, rows, sends, faces, place, cell_refs):
    depth = field.depth
    for buffer, b, y in ((faces[0], 1, rows - 1), (faces[1], -1, 0)):
        for a in (-1, 0, 1):
            for e in (-1, 0, 1):
                k = 9 * (a + 1) + 3 * (b + 1) + e + 1
                first = (3 * (a + 1) + e + 1) * depth
                for x in range(depth):
                    buffer[first + x : first + x + 1, :] = field[k, x, slice(y, y + 1), slice(None)]
        for i, ref in enumerate(cell_refs):
            for x in range(depth):
                at = (9 + i) * depth + x
                buffer[at : at + 1, :] = ref[x, y : y + 1, :].astype(jnp.float32)
    even = place[1] == 0

    @pl.when(even)
    def _():
        sends[0][...] = faces[0][...]
        sends[1][...] = faces[1][...]

    @pl.when(jnp.logical_not(even))
    def _():
        sends[0][...] = faces[1][...]
        sends[1][...] = faces[0][...]


def unpack_y(pairs, corner, low, high, corner_low, corner_high, place):
    even = place[1] == 0

    def take(first, second):
        first[0][...] = pairs[0][...]
        second[0][...] = pairs[1][...]
        if corner is not None:
            for side in range(2):
                first[1][side] = corner[side, 0:8, :]
                second[1][side] = corner[side, 8:16, :]

    @pl.when(even)
    def _():
        take((high, corner_high), (low, corner_low))

    @pl.when(jnp.logical_not(even))
    def _():
        take((low, corner_low), (high, corner_high))


def corner_kernel(first, second, out, *, depth, extra):
    for side, a, x in ((0, 1, depth - 1), (1, -1, 0)):
        for p, ref in enumerate((first, second)):
            for e in range(3):
                at = (3 * (a + 1) + e) * depth + x
                out[side, 8 * p + e : 8 * p + e + 1, :] = ref[at : at + 1, :]
            for i in range(extra):
                at = (9 + i) * depth + x
                out[side, 8 * p + 3 + i : 8 * p + 4 + i, :] = ref[at : at + 1, :]


def collide_all(source, rates, target):
    def body(x, span):
        raw = along_axes([source[k, x, :, span] for k in range(27)], to_moment)
        equal = equilibrium_terms(*density_velocity(raw))
        values = along_axes(relaxed(raw, equal, rates), from_moment)
        for k in range(27):
            target[k, x, :, span] = values[k]

    return body


def first_edge_kernel(populations, kind, profile, rates, edge, send_x):
    body = collide_all(populations, rates, edge)
    for start in range(0, populations.shape[3], LANES):
        body(0, slice(start, start + LANES))
    base = 18 * pl.program_id(0)
    for i in range(9):
        send_x[0, i] = edge[base + i, 0]
    send_x[0, 9] = kind[0].astype(jnp.float32)
    send_x[0, 10] = profile[0].astype(jnp.float32)


def first_inner_kernel(populations, edge, kind, profile, rates, place, inner, *rest):
    sends, faces = rest[:2], rest[2:]
    depth, rows, cells = populations.shape[1:]

    def plane(x, carry):
        for start in range(0, cells, LANES):
            span = slice(start, start + LANES)
            raw = along_axes([populations[k, x + 1, :, span] for k in range(27)], to_moment)
            equal = equilibrium_terms(*density_velocity(raw))
            values = along_axes(relaxed(raw, equal, rates), from_moment)
            for k in range(27):
                inner[k, x, :, span] = values[k]
        return carry

    lax.fori_loop(0, depth - 2, plane, 0)
    pack_y(Planes(edge, inner), rows, sends, faces, place, (kind, profile))


def shifted(plane, row, b, e, sublane):
    rows, cells = plane.shape
    if b:
        plane = pltpu.roll(plane, b % rows, 0)
        edge = 0 if b == 1 else rows - 1
        plane = jnp.where(sublane == edge, jnp.broadcast_to(row, plane.shape), plane)
    if e:
        plane = pltpu.roll(plane, e % cells, 1)
    return plane


def cell_fields(kind, profile, table):
    open_cell = (kind == 0) | (kind >= 3)
    vent = kind == 2
    velocity = vent_velocity(profile, table)
    return [jnp.where(open_cell, OPEN, 0.0)] + [jnp.where(vent, 6.0 * v, 0.0) for v in velocity]


def make_fields(halo, kind, profile, table, place, kinds_row, profiles_row, planes, edges, span):
    recv_x, recv_low, recv_high, corner_low, corner_high = halo
    depth = kind.shape[0]
    for x in span:
        if 0 <= x < depth:
            kinds, profiles = kind[x].astype(jnp.float32), profile[x].astype(jnp.float32)
        else:
            side = 0 if x < 0 else 1
            kinds, profiles = recv_x[side, 9], recv_x[side, 10]
        for c, value in enumerate(cell_fields(kinds, profiles, table)):
            planes[c, x + 1] = value
    row_sides = ((recv_low, corner_low, 0), (recv_high, corner_high, PY - 1))
    for s, (buffer, corner, outer) in enumerate(row_sides):
        for target, i in ((kinds_row, 0), (profiles_row, 1)):
            target[...] = jnp.zeros(target.shape, jnp.float32)
            at = (9 + i) * depth
            for x in range(depth):
                target[x + 1 : x + 2, :] = buffer[at + x : at + x + 1, :]
            if -1 in span:
                target[0:1, :] = corner[0, 3 + i : 4 + i, :]
                target[depth + 1 : depth + 2, :] = corner[1, 3 + i : 4 + i, :]
        kinds = jnp.where(place[0] == outer, 1.0, kinds_row[...])
        for c, value in enumerate(cell_fields(kinds, profiles_row[...], table)):
            edges[s, c] = value


def stream(field, halo, bounce, passed, fields, targets, shape):
    recv_x, recv_low, recv_high, corner_low, corner_high = halo
    depth, rows, cells = shape
    sublane = lax.broadcasted_iota(jnp.int32, (rows, cells), 0)
    lane = lax.broadcasted_iota(jnp.int32, (rows, cells), 1)
    for k in range(27):
        a, b, e = direction(k)
        for at_x, x in enumerate(targets):
            if k == 13:
                passed[k, at_x] = field[k, x]
                continue
            source = x - a
            side = 0 if source < 0 else 1
            inside = 0 <= source < depth
            plane = field[k, source] if inside else recv_x[side, 3 * (b + 1) + e + 1]
            row = None
            if b:
                buffer, corner = (recv_low, corner_low) if b == 1 else (recv_high, corner_high)
                at = (3 * (a + 1) + e + 1) * depth + source
                row = buffer[at : at + 1, :] if inside else corner[side, e + 1 : e + 2, :]
            if fields is not None:
                planes, edges = fields

                def combine(read):
                    value = read(0)
                    for c, step in enumerate((a, b, e)):
                        if step:
                            value = value + read(c + 1) if step > 0 else value - read(c + 1)
                    return value

                term = combine(lambda c: planes[c, source + 1])
                term_row = None
                if b:
                    s = 0 if b == 1 else 1
                    term_row = combine(lambda c: edges[s, c, source + 1 : source + 2, :])
                term = shifted(term, term_row, b, e, sublane)
                if e:
                    term = jnp.where(lane == (0 if e == 1 else cells - 1), 0.0, term)
                bounce[k, at_x] = term
            term = bounce[k, at_x]
            value = shifted(plane, row, b, e, sublane)
            passed[k, at_x] = jnp.where(term > 0.5 * OPEN, value, field[26 - k, x] + term)


def chosen(kind, profile, table, velocity):
    vent = vent_velocity(profile, table)
    return [
        jnp.where(kind == 3, vent[c], jnp.where(kind == 4, velocity[c], 0.0)) for c in range(3)
    ]


def collide_cells(passed, kind, profile, table, rates, collided, base, stride):
    count, cells = passed.shape[1], passed.shape[3]

    def body(x, span):
        kinds = kind[base + x * stride, :, span]
        fluid = kinds == 0
        raw = along_axes([passed[k, x, :, span] for k in range(27)], to_moment)
        density, velocity = density_velocity(raw)
        forced = chosen(kinds, profile[base + x * stride, :, span], table, velocity)
        density = jnp.where(fluid, density, 1.0)
        velocity = [jnp.where(fluid, velocity[c], forced[c]) for c in range(3)]
        equal = equilibrium_terms(density, velocity)
        mixed = relaxed(raw, equal, rates)
        values = [jnp.where(fluid, mixed[k], equal[k]) for k in range(27)]
        values = along_axes(values, from_moment)
        for k in range(27):
            collided[k, x, :, span] = values[k]

    tiles(count, cells, body)


def finish_cells(passed, kind, profile, table, advanced, base, stride, out_base, out_stride):
    count, cells = passed.shape[1], passed.shape[3]

    def body(x, span):
        kinds = kind[base + x * stride, :, span]
        fluid = kinds == 0
        values = [passed[k, x, :, span] for k in range(27)]
        velocity = density_velocity(along_axes(values, to_moment))[1]
        ux, uy, uz = chosen(kinds, profile[base + x * stride, :, span], table, velocity)
        rest = 1.0 - 1.5 * (ux * ux + uy * uy + uz * uz)
        for k in range(27):
            projected = None
            for step, u in zip(direction(k), (ux, uy, uz)):
                if step:
                    signed = u if step > 0 else -u
                    projected = signed if projected is None else projected + signed
            equal = rest if projected is None else rest + projected * (3.0 + 4.5 * projected)
            advanced[k, out_base + x * out_stride, :, span] = jnp.where(fluid, values[k], equal)

    tiles(count, cells, body)


def inner_kernel(*refs, fresh, last):
    refs = list(refs)
    edge, inner, first, second = refs[:4]
    del refs[:4]
    bounce = None if fresh else refs.pop(0)
    kind, profile, table, rates, place, out = refs[:6]
    del refs[:6]
    if fresh:
        bounce = refs.pop(0)
    passed, low, high = refs[:3]
    depth, rows, cells = kind.shape
    unpack_y((first, second), None, low, high, None, None, place)
    halo = (None, low, high, None, None)
    fields = None
    if fresh:
        kinds_row, profiles_row, planes, edges = refs[3:]
        make_fields(
            halo, kind, profile, table, place, kinds_row, profiles_row, planes, edges, range(depth)
        )
        fields = (planes, edges)
    targets = range(1, depth - 1)
    stream(Planes(edge, inner), halo, bounce, passed, fields, targets, kind.shape)
    if last:
        finish_cells(passed, kind, profile, table, out, 1, 1, 0, 1)
    else:
        collide_cells(passed, kind, profile, table, rates, out, 1, 1)


def edge_kernel(*refs, fresh, last):
    refs = list(refs)
    edge, inner, next_inner, recv_x, first, second, corner = refs[:7]
    del refs[:7]
    bounce = None if fresh else refs.pop(0)
    kind, profile, table, rates, place, out = refs[:6]
    del refs[:6]
    if fresh:
        bounce = refs.pop(0)
    if not last:
        send_x, send_first, send_second = refs[:3]
        del refs[:3]
    passed, low, high, corner_low, corner_high = refs[:5]
    del refs[:5]
    depth, rows, cells = kind.shape
    unpack_y((first, second), corner, low, high, corner_low, corner_high, place)
    halo = (recv_x, low, high, corner_low, corner_high)
    fields = None
    if fresh:
        kinds_row, profiles_row, planes, edges = refs[:4]
        del refs[:4]
        make_fields(
            halo, kind, profile, table, place, kinds_row, profiles_row, planes, edges,
            range(-1, depth + 1),
        )
        fields = (planes, edges)
    targets = (0, depth - 1)
    stream(Planes(edge, inner), halo, bounce, passed, fields, targets, kind.shape)
    if last:
        finish_cells(passed, kind, profile, table, out, 0, depth - 1, 0, depth - 1)
        for k in range(27):
            for x in range(1, depth - 1):
                out[k, x] = next_inner[k, x - 1]
        return
    collide_cells(passed, kind, profile, table, rates, out, 0, depth - 1)
    pack_x(out, send_x, ())
    pack_y(Planes(out, next_inner), rows, (send_first, send_second), refs, place, ())


def passed_along(value, steps):
    count = lax.axis_size("gx")
    pairs = [(source, (source + steps) % count) for source in range(count)]
    return lax.ppermute(value, "gx", pairs)


def swapped(value, parity):
    count = lax.axis_size("gx")
    pairs = []
    for source in range(parity, count, 2):
        target = (source + 1) % count
        if (target + PY // 2) % PY:
            pairs += [(source, target), (target, source)]
    return lax.ppermute(value, "gx", pairs)


def both_sides(value):
    if lax.axis_size("gx") == 2 * PY:
        return passed_along(value, PY)
    return jnp.stack([passed_along(value[0], PY), passed_along(value[1], -PY)])


def round_up(value, step):
    return -(-value // step) * step


def local(populations, cell_kind, profile, vent_table, rates):
    scaled = populations[:, 0]
    kind, profile = cell_kind[0], profile[0]
    depth, rows, cells = kind.shape
    f32 = jnp.float32
    vmem = pl.BlockSpec(memory_space=pltpu.VMEM)
    smem = pl.BlockSpec(memory_space=pltpu.SMEM)
    index = lax.axis_index("gx")
    place = jnp.stack([(index + PY // 2) % PY, index % 2]).astype(jnp.int32)

    def array(*shape):
        return jax.ShapeDtypeStruct(shape, f32)

    def scratch(*shape):
        return pltpu.VMEM(shape, f32)

    def call(body, specs, outs, scratch_shapes, name, **options):
        return pl.pallas_call(
            functools.partial(body, **options) if options else body,
            in_specs=specs,
            out_specs=jax.tree.map(lambda _: vmem, outs),
            out_shape=outs,
            scratch_shapes=scratch_shapes,
            name=name,
        )

    edge_shape, inner_shape = (27, 2, rows, cells), (27, depth - 2, rows, cells)
    wide = (round_up(11 * depth, 8), cells)
    narrow = (round_up(9 * depth, 8), cells)
    line = round_up(depth + 2, 8)
    field_scratch = [
        scratch(line, cells),
        scratch(line, cells),
        scratch(4, depth + 2, rows, cells),
        scratch(2, 4, line, cells),
    ]
    corners = [scratch(2, 8, cells)] * 2

    plane_at = lambda i: (i * (depth - 1), 0, 0)
    edge, send_x = pl.pallas_call(
        first_edge_kernel,
        grid=(2,),
        in_specs=[
            pl.BlockSpec((27, 1, rows, cells), lambda i: (0, i * (depth - 1), 0, 0)),
            pl.BlockSpec((1, rows, cells), plane_at),
            pl.BlockSpec((1, rows, cells), plane_at),
            smem,
        ],
        out_specs=(
            pl.BlockSpec((27, 1, rows, cells), lambda i: (0, i, 0, 0)),
            pl.BlockSpec((1, 11, rows, cells), lambda i: (1 - i, 0, 0, 0)),
        ),
        out_shape=(array(*edge_shape), array(2, 11, rows, cells)),
        name="first_edge",
    )(scaled, kind, profile, rates)
    recv_x = both_sides(send_x)
    inner, *sends = call(
        first_inner_kernel,
        [vmem] * 4 + [smem] * 2,
        (array(*inner_shape), array(*wide), array(*wide)),
        [scratch(*wide)] * 2,
        "first_inner",
    )(scaled, edge, kind, profile, rates, place)
    shared = (kind, profile, vent_table, rates, place)
    shared_specs = [vmem] * 2 + [smem] * 3
    inner_bounce = edge_bounce = None
    for step in range(STEPS):
        fresh, last = step == 0, step == STEPS - 1
        extra = 2 if fresh else 0
        shape = wide if fresh else narrow
        pairs = swapped(sends[0], 0), swapped(sends[1], 1)
        corner = call(
            corner_kernel, [vmem] * 2, array(2, 16, cells), [], "corner", depth=depth, extra=extra
        )(*pairs)
        corner = both_sides(corner)
        outs = [array(*inner_shape)] + ([array(*inner_shape)] if fresh else [])
        known = () if fresh else (inner_bounce,)
        results = call(
            inner_kernel,
            [vmem] * (4 + len(known)) + shared_specs,
            tuple(outs),
            [scratch(*inner_shape)] + [scratch(*shape)] * 2 + (field_scratch if fresh else []),
            "inner",
            fresh=fresh,
            last=last,
        )(edge, inner, *pairs, *known, *shared)
        next_inner = results[0]
        if fresh:
            inner_bounce = results[1]
        outs = [array(27, depth, rows, cells) if last else array(*edge_shape)]
        outs += [array(*edge_shape)] if fresh else []
        outs += [] if last else [array(2, 9, rows, cells), array(*narrow), array(*narrow)]
        known = () if fresh else (edge_bounce,)
        results = list(
            call(
                edge_kernel,
                [vmem] * (7 + len(known)) + shared_specs,
                tuple(outs),
                [scratch(*edge_shape)]
                + [scratch(*shape)] * 2
                + corners
                + (field_scratch if fresh else [])
                + ([] if last else [scratch(*narrow)] * 2),
                "edge",
                fresh=fresh,
                last=last,
            )(edge, inner, next_inner, recv_x, *pairs, corner, *known, *shared)
        )
        edge = results.pop(0)
        inner = next_inner
        if fresh:
            edge_bounce = results.pop(0)
        if not last:
            recv_x = both_sides(results.pop(0))
            sends = results
    return edge[:, None]


def solution(mesh):
    return jax.shard_map(
        local,
        mesh=mesh,
        in_specs=(
            P("scen", "gx", None, None, None),
            P("gx", None, None, "scen"),
            P("gx", None, None, "scen"),
            P("scen", None),
            P(),
        ),
        out_specs=P("scen", "gx", None, None, None),
        check_vma=False,
    )
```

```python
import functools

import jax
import jax.numpy as jnp
import numpy as np
from jax import lax
from jax.experimental import pallas as pl
from jax.experimental.pallas import tpu as pltpu
from jax.sharding import PartitionSpec as P

PY = 8
STEPS = 3
LANES = 128
OPEN = 1e30
CONSERVED = (0, 9, 3, 1)


def direction(k):
    return k // 9 - 1, k // 3 % 3 - 1, k % 3 - 1


def equilibrium_moments():
    speeds = np.array([direction(k) for k in range(27)], float)
    single = np.array([1.0 / 6.0, 2.0 / 3.0, 1.0 / 6.0])
    weights = np.kron(np.kron(single, single), single)
    powers = np.array([[1.0, 1.0, 1.0], [-1.0, 0.0, 1.0], [1.0, 0.0, 1.0]])
    moments = np.kron(np.kron(powers, powers), powers)
    basis = [np.ones(27)]
    basis += [3.0 * speeds[:, i] for i in range(3)]
    basis += [4.5 * speeds[:, i] ** 2 - 1.5 for i in range(3)]
    basis += [9.0 * speeds[:, i] * speeds[:, j] for i, j in ((0, 1), (0, 2), (1, 2))]
    return 27.0 * moments @ (weights[:, None] * np.stack(basis, 1))


TABLE = equilibrium_moments()


def along_axes(values, change):
    for stride in (9, 3, 1):
        out = list(values)
        for k in range(27):
            if k // stride % 3 == 0:
                trio = (values[k], values[k + stride], values[k + 2 * stride])
                out[k], out[k + stride], out[k + 2 * stride] = change(*trio)
        values = out
    return values


def to_moment(low, mid, high):
    total = low + high
    return total + 4.0 * mid, high - low, total


def from_moment(zeroth, first, second):
    return second - first, 0.5 * (zeroth - second), first + second


def equilibrium_terms(density, velocity):
    ux, uy, uz = velocity
    jx, jy, jz = density * ux, density * uy, density * uz
    terms = (density, jx, jy, jz, jx * ux, jy * uy, jz * uz, jx * uy, jx * uz, jy * uz)
    result = []
    for k in range(27):
        value = None
        for t in range(10):
            coefficient = float(TABLE[k, t])
            if abs(coefficient) > 1e-9:
                piece = terms[t] if abs(coefficient - 1.0) < 1e-9 else coefficient * terms[t]
                value = piece if value is None else value + piece
        result.append(jnp.zeros_like(density) if value is None else value)
    return result


def density_velocity(raw):
    inverse = 1.0 / raw[0]
    return raw[0] * (1.0 / 216.0), (raw[9] * inverse, raw[3] * inverse, raw[1] * inverse)


def vent_velocity(profile, table_ref):
    parts = [jnp.zeros(profile.shape, jnp.float32) for _ in range(3)]
    for p in range(table_ref.shape[0]):
        match = profile == p
        parts = [jnp.where(match, table_ref[p, c], parts[c]) for c in range(3)]
    return parts


def relaxed(raw, equal, rates_ref):
    result = []
    for k in range(27):
        if k in CONSERVED:
            result.append(0.125 * raw[k])
        else:
            rate = rates_ref[k]
            result.append(rate * equal[k] + ((1.0 - rate) * 0.125) * raw[k])
    return result


def tiles(depth, cells, body):
    def plane(x, carry):
        for start in range(0, cells, LANES):
            body(x, slice(start, start + LANES))
        return carry

    lax.fori_loop(0, depth, plane, 0)


def by_parity(place, even_case, odd_case):
    for wanted, pairs in ((0, even_case), (1, odd_case)):

        @pl.when(place[1] == wanted)
        def _():
            for target, source in pairs:
                target[...] = source[...]


def unpack(received, ordered, place):
    recv_x, first, second, corner_first, corner_second = received
    low, high, corner_low, corner_high = ordered
    by_parity(
        place,
        ((high, first), (low, second), (corner_high, corner_first), (corner_low, corner_second)),
        ((low, first), (high, second), (corner_low, corner_first), (corner_high, corner_second)),
    )
    return recv_x, low, high, corner_low, corner_high


def pack(collided, sends, faces, place, cell_refs):
    send_x, first_send, second_send, first_corner, second_corner = sends
    send_up, send_down, corner_up, corner_down = faces
    depth, rows = collided.shape[1], collided.shape[2]
    for side, a, x in ((0, 1, depth - 1), (1, -1, 0)):
        for i in range(9):
            send_x[side, i] = collided[9 * (a + 1) + i, x]
        for i, ref in enumerate(cell_refs):
            send_x[side, 9 + i] = ref[x].astype(jnp.float32)
    for buffer, corner, b, y in ((send_up, corner_up, 1, rows - 1), (send_down, corner_down, -1, 0)):
        for a in (-1, 0, 1):
            for e in (-1, 0, 1):
                k = 9 * (a + 1) + 3 * (b + 1) + e + 1
                first = (3 * (a + 1) + e + 1) * depth
                for x in range(depth):
                    buffer[first + x : first + x + 1, :] = collided[k, x, y : y + 1, :]
        for i, ref in enumerate(cell_refs):
            for x in range(depth):
                at = (9 + i) * depth + x
                buffer[at : at + 1, :] = ref[x, y : y + 1, :].astype(jnp.float32)
        for side, a, x in ((0, 1, depth - 1), (1, -1, 0)):
            for e in (-1, 0, 1):
                k = 9 * (a + 1) + 3 * (b + 1) + e + 1
                corner[side, e + 1 : e + 2, :] = collided[k, x, y : y + 1, :]
            for i, ref in enumerate(cell_refs):
                corner[side, 3 + i : 4 + i, :] = ref[x, y : y + 1, :].astype(jnp.float32)
    by_parity(
        place,
        (
            (first_send, send_up),
            (second_send, send_down),
            (first_corner, corner_up),
            (second_corner, corner_down),
        ),
        (
            (first_send, send_down),
            (second_send, send_up),
            (first_corner, corner_down),
            (second_corner, corner_up),
        ),
    )


def first_kernel(populations, kind, profile, rates, place, collided, *rest):
    sends, faces = rest[:5], rest[5:]
    depth, cells = populations.shape[1], populations.shape[3]

    def body(x, span):
        raw = along_axes([populations[k, x, :, span] for k in range(27)], to_moment)
        equal = equilibrium_terms(*density_velocity(raw))
        values = along_axes(relaxed(raw, equal, rates), from_moment)
        for k in range(27):
            collided[k, x, :, span] = values[k]

    tiles(depth, cells, body)
    pack(collided, sends, faces, place, (kind, profile))


def shifted(plane, row, b, e, sublane):
    rows, cells = plane.shape
    if b:
        plane = pltpu.roll(plane, b % rows, 0)
        edge = 0 if b == 1 else rows - 1
        plane = jnp.where(sublane == edge, jnp.broadcast_to(row, plane.shape), plane)
    if e:
        plane = pltpu.roll(plane, e % cells, 1)
    return plane


def cell_fields(kind, profile, table):
    open_cell = (kind == 0) | (kind >= 3)
    vent = kind == 2
    velocity = vent_velocity(profile, table)
    return [jnp.where(open_cell, OPEN, 0.0)] + [jnp.where(vent, 6.0 * v, 0.0) for v in velocity]


def make_fields(halo, kind, profile, table, place, kinds_row, profiles_row, planes, edges):
    recv_x, recv_low, recv_high, corner_low, corner_high = halo
    depth = kind.shape[0]
    for x in range(-1, depth + 1):
        if 0 <= x < depth:
            kinds, profiles = kind[x].astype(jnp.float32), profile[x].astype(jnp.float32)
        else:
            side = 0 if x < 0 else 1
            kinds, profiles = recv_x[side, 9], recv_x[side, 10]
        for c, value in enumerate(cell_fields(kinds, profiles, table)):
            planes[c, x + 1] = value
    row_sides = ((recv_low, corner_low, 0), (recv_high, corner_high, PY - 1))
    for s, (buffer, corner, outer) in enumerate(row_sides):
        for target, i in ((kinds_row, 0), (profiles_row, 1)):
            target[...] = jnp.zeros(target.shape, jnp.float32)
            target[0:1, :] = corner[0, 3 + i : 4 + i, :]
            at = (9 + i) * depth
            for x in range(depth):
                target[x + 1 : x + 2, :] = buffer[at + x : at + x + 1, :]
            target[depth + 1 : depth + 2, :] = corner[1, 3 + i : 4 + i, :]
        kinds = jnp.where(place[0] == outer, 1.0, kinds_row[...])
        for c, value in enumerate(cell_fields(kinds, profiles_row[...], table)):
            edges[s, c] = value


def stream(collided, halo, bounce, passed, fields):
    recv_x, recv_low, recv_high, corner_low, corner_high = halo
    depth, rows, cells = collided.shape[1:]
    sublane = lax.broadcasted_iota(jnp.int32, (rows, cells), 0)
    lane = lax.broadcasted_iota(jnp.int32, (rows, cells), 1)
    for k in range(27):
        a, b, e = direction(k)
        for x in range(depth):
            if k == 13:
                passed[k, x] = collided[k, x]
                continue
            source = x - a
            side = 0 if source < 0 else 1
            inside = 0 <= source < depth
            plane = collided[k, source] if inside else recv_x[side, 3 * (b + 1) + e + 1]
            row = None
            if b:
                buffer, corner = (recv_low, corner_low) if b == 1 else (recv_high, corner_high)
                at = (3 * (a + 1) + e + 1) * depth + source
                row = buffer[at : at + 1, :] if inside else corner[side, e + 1 : e + 2, :]
            if fields is not None:
                planes, edges = fields

                def combine(read):
                    value = read(0)
                    for c, step in enumerate((a, b, e)):
                        if step:
                            value = value + read(c + 1) if step > 0 else value - read(c + 1)
                    return value

                term = combine(lambda c: planes[c, source + 1])
                term_row = None
                if b:
                    s = 0 if b == 1 else 1
                    term_row = combine(lambda c: edges[s, c, source + 1 : source + 2, :])
                term = shifted(term, term_row, b, e, sublane)
                if e:
                    term = jnp.where(lane == (0 if e == 1 else cells - 1), 0.0, term)
                bounce[k, x] = term
            term = bounce[k, x]
            value = shifted(plane, row, b, e, sublane)
            passed[k, x] = jnp.where(term > 0.5 * OPEN, value, collided[26 - k, x] + term)


def chosen(kind, profile, table, velocity):
    vent = vent_velocity(profile, table)
    return [
        jnp.where(kind == 3, vent[c], jnp.where(kind == 4, velocity[c], 0.0)) for c in range(3)
    ]


def collide_cells(passed, kind, profile, table, rates, collided):
    depth, cells = passed.shape[1], passed.shape[3]

    def body(x, span):
        kinds = kind[x, :, span]
        fluid = kinds == 0
        raw = along_axes([passed[k, x, :, span] for k in range(27)], to_moment)
        density, velocity = density_velocity(raw)
        forced = chosen(kinds, profile[x, :, span], table, velocity)
        density = jnp.where(fluid, density, 1.0)
        velocity = [jnp.where(fluid, velocity[c], forced[c]) for c in range(3)]
        equal = equilibrium_terms(density, velocity)
        mixed = relaxed(raw, equal, rates)
        values = [jnp.where(fluid, mixed[k], equal[k]) for k in range(27)]
        values = along_axes(values, from_moment)
        for k in range(27):
            collided[k, x, :, span] = values[k]

    tiles(depth, cells, body)


def finish_cells(passed, kind, profile, table, advanced):
    depth, cells = passed.shape[1], passed.shape[3]

    def body(x, span):
        kinds = kind[x, :, span]
        fluid = kinds == 0
        values = [passed[k, x, :, span] for k in range(27)]
        velocity = density_velocity(along_axes(values, to_moment))[1]
        ux, uy, uz = chosen(kinds, profile[x, :, span], table, velocity)
        base = 1.0 - 1.5 * (ux * ux + uy * uy + uz * uz)
        for k in range(27):
            projected = None
            for step, u in zip(direction(k), (ux, uy, uz)):
                if step:
                    signed = u if step > 0 else -u
                    projected = signed if projected is None else projected + signed
            equal = base if projected is None else base + projected * (3.0 + 4.5 * projected)
            advanced[k, x, :, span] = jnp.where(fluid, values[k], equal)

    tiles(depth, cells, body)


def second_kernel(*refs):
    collided, *received = refs[:6]
    kind, profile, table, rates, place = refs[6:11]
    out, bounce = refs[11:13]
    sends = refs[13:18]
    passed, kinds_row, profiles_row, planes, edges = refs[18:23]
    halo = unpack(received, refs[23:27], place)
    make_fields(halo, kind, profile, table, place, kinds_row, profiles_row, planes, edges)
    stream(collided, halo, bounce, passed, (planes, edges))
    collide_cells(passed, kind, profile, table, rates, out)
    pack(out, sends, refs[27:], place, ())


def middle_kernel(*refs):
    collided, *received = refs[:6]
    bounce, kind, profile, table, rates, place = refs[6:12]
    out = refs[12]
    sends = refs[13:18]
    passed = refs[18]
    halo = unpack(received, refs[19:23], place)
    stream(collided, halo, bounce, passed, None)
    collide_cells(passed, kind, profile, table, rates, out)
    pack(out, sends, refs[23:], place, ())


def last_kernel(*refs):
    collided, *received = refs[:6]
    bounce, kind, profile, table, place, advanced, passed = refs[6:13]
    halo = unpack(received, refs[13:], place)
    stream(collided, halo, bounce, passed, None)
    finish_cells(passed, kind, profile, table, advanced)


def passed_along(value, steps):
    count = lax.axis_size("gx")
    pairs = [(source, (source + steps) % count) for source in range(count)]
    return lax.ppermute(value, "gx", pairs)


def swapped(value, parity, across):
    count = lax.axis_size("gx")
    pairs = []
    for source in range(parity, count, 2):
        target = (source + 1) % count
        if (target + PY // 2) % PY:
            pairs.append((source, (target + across) % count))
            pairs.append((target, (source + across) % count))
    return lax.ppermute(value, "gx", pairs)


def both_sides(value, send):
    if lax.axis_size("gx") == 2 * PY:
        return send(value, PY)
    return jnp.stack([send(value[0], PY), send(value[1], -PY)])


def exchange(sends):
    send_x, first, second, corner_first, corner_second = sends
    return (
        both_sides(send_x, passed_along),
        swapped(first, 0, 0),
        swapped(second, 1, 0),
        both_sides(corner_first, lambda value, across: swapped(value, 0, across)),
        both_sides(corner_second, lambda value, across: swapped(value, 1, across)),
    )


def round_up(value, step):
    return -(-value // step) * step


def local(populations, cell_kind, profile, vent_table, rates):
    scaled = populations[:, 0]
    kind, profile = cell_kind[0], profile[0]
    depth, rows, cells = kind.shape
    f32 = jnp.float32
    field = jax.ShapeDtypeStruct(scaled.shape, f32)
    vmem = pl.BlockSpec(memory_space=pltpu.VMEM)
    smem = pl.BlockSpec(memory_space=pltpu.SMEM)
    index = lax.axis_index("gx")
    place = jnp.stack([(index + PY // 2) % PY, index % 2]).astype(jnp.int32)

    def send_shapes(extra):
        along = jax.ShapeDtypeStruct((round_up((9 + extra) * depth, 8), cells), f32)
        corner = jax.ShapeDtypeStruct((2, 8, cells), f32)
        across = jax.ShapeDtypeStruct((2, 9 + extra, rows, cells), f32)
        return (across, along, along, corner, corner)

    def ordered(extra):
        return [pltpu.VMEM(shape.shape, f32) for shape in send_shapes(extra)[1:]]

    def call(body, specs, outs, scratch, name):
        return pl.pallas_call(
            body,
            in_specs=specs,
            out_specs=jax.tree.map(lambda _: vmem, outs),
            out_shape=outs,
            scratch_shapes=scratch,
            name=name,
        )

    buffer = pltpu.VMEM(scaled.shape, f32)
    edge_rows = round_up(depth + 2, 8)
    collided, *sends = call(
        first_kernel, [vmem] * 3 + [smem] * 2, (field,) + send_shapes(2), ordered(2), "first"
    )(scaled, kind, profile, rates, place)
    halo = exchange(sends)
    collided, bounce, *sends = call(
        second_kernel,
        [vmem] * 8 + [smem] * 3,
        (field, field) + send_shapes(0),
        [
            buffer,
            pltpu.VMEM((edge_rows, cells), f32),
            pltpu.VMEM((edge_rows, cells), f32),
            pltpu.VMEM((4, depth + 2, rows, cells), f32),
            pltpu.VMEM((2, 4, edge_rows, cells), f32),
        ]
        + ordered(2)
        + ordered(0),
        "second",
    )(collided, *halo, kind, profile, vent_table, rates, place)
    for _ in range(STEPS - 2):
        halo = exchange(sends)
        collided, *sends = call(
            middle_kernel,
            [vmem] * 9 + [smem] * 3,
            (field,) + send_shapes(0),
            [buffer] + ordered(0) * 2,
            "middle",
        )(collided, *halo, bounce, kind, profile, vent_table, rates, place)
    halo = exchange(sends)
    advanced = call(
        last_kernel, [vmem] * 9 + [smem] * 2, field, [buffer] + ordered(0), "last"
    )(collided, *halo, bounce, kind, profile, vent_table, place)
    return advanced[:, None]


def solution(mesh):
    return jax.shard_map(
        local,
        mesh=mesh,
        in_specs=(
            P("scen", "gx", None, None, None),
            P("gx", None, None, "scen"),
            P("gx", None, None, "scen"),
            P("scen", None),
            P(),
        ),
        out_specs=P("scen", "gx", None, None, None),
        check_vma=False,
    )
```

```python
import functools

import jax
import jax.numpy as jnp
import numpy as np
from jax import lax
from jax.experimental import pallas as pl
from jax.experimental.pallas import tpu as pltpu
from jax.sharding import PartitionSpec as P

PY = 8
STEPS = 3
LANES = 128
OPEN = 1e30
CONSERVED = (0, 9, 3, 1)


def direction(k):
    return k // 9 - 1, k // 3 % 3 - 1, k % 3 - 1


def equilibrium_moments():
    speeds = np.array([direction(k) for k in range(27)], float)
    single = np.array([1.0 / 6.0, 2.0 / 3.0, 1.0 / 6.0])
    weights = np.kron(np.kron(single, single), single)
    powers = np.array([[1.0, 1.0, 1.0], [-1.0, 0.0, 1.0], [1.0, 0.0, 1.0]])
    moments = np.kron(np.kron(powers, powers), powers)
    basis = [np.ones(27)]
    basis += [3.0 * speeds[:, i] for i in range(3)]
    basis += [4.5 * speeds[:, i] ** 2 - 1.5 for i in range(3)]
    basis += [9.0 * speeds[:, i] * speeds[:, j] for i, j in ((0, 1), (0, 2), (1, 2))]
    return 27.0 * moments @ (weights[:, None] * np.stack(basis, 1))


TABLE = equilibrium_moments()


def along_axes(values, change):
    for stride in (9, 3, 1):
        out = list(values)
        for k in range(27):
            if k // stride % 3 == 0:
                trio = (values[k], values[k + stride], values[k + 2 * stride])
                out[k], out[k + stride], out[k + 2 * stride] = change(*trio)
        values = out
    return values


def to_moment(low, mid, high):
    total = low + high
    return total + 4.0 * mid, high - low, total


def from_moment(zeroth, first, second):
    return second - first, 0.5 * (zeroth - second), first + second


def equilibrium_terms(density, velocity):
    ux, uy, uz = velocity
    jx, jy, jz = density * ux, density * uy, density * uz
    terms = (density, jx, jy, jz, jx * ux, jy * uy, jz * uz, jx * uy, jx * uz, jy * uz)
    result = []
    for k in range(27):
        value = None
        for t in range(10):
            coefficient = float(TABLE[k, t])
            if abs(coefficient) > 1e-9:
                piece = terms[t] if abs(coefficient - 1.0) < 1e-9 else coefficient * terms[t]
                value = piece if value is None else value + piece
        result.append(jnp.zeros_like(density) if value is None else value)
    return result


def density_velocity(raw):
    inverse = 1.0 / raw[0]
    return raw[0] * (1.0 / 216.0), (raw[9] * inverse, raw[3] * inverse, raw[1] * inverse)


def vent_velocity(profile, table_ref):
    parts = [jnp.zeros(profile.shape, jnp.float32) for _ in range(3)]
    for p in range(table_ref.shape[0]):
        match = profile == p
        parts = [jnp.where(match, table_ref[p, c], parts[c]) for c in range(3)]
    return parts


def relaxed(raw, equal, rates_ref):
    result = []
    for k in range(27):
        if k in CONSERVED:
            result.append(0.125 * raw[k])
        else:
            rate = rates_ref[k]
            result.append(rate * equal[k] + ((1.0 - rate) * 0.125) * raw[k])
    return result


def tiles(depth, cells, body):
    def plane(x, carry):
        for start in range(0, cells, LANES):
            body(x, slice(start, start + LANES))
        return carry

    lax.fori_loop(0, depth, plane, 0)


def pack(collided, sends, cell_refs):
    send_x, send_up, send_down, corner_up, corner_down = sends
    depth, rows = collided.shape[1], collided.shape[2]
    for side, a, x in ((0, 1, depth - 1), (1, -1, 0)):
        for i in range(9):
            send_x[side, i] = collided[9 * (a + 1) + i, x]
        for i, ref in enumerate(cell_refs):
            send_x[side, 9 + i] = ref[x].astype(jnp.float32)
    for buffer, corner, b, y in ((send_up, corner_up, 1, rows - 1), (send_down, corner_down, -1, 0)):
        for a in (-1, 0, 1):
            for e in (-1, 0, 1):
                k = 9 * (a + 1) + 3 * (b + 1) + e + 1
                first = (3 * (a + 1) + e + 1) * depth
                for x in range(depth):
                    buffer[first + x : first + x + 1, :] = collided[k, x, y : y + 1, :]
        for i, ref in enumerate(cell_refs):
            for x in range(depth):
                at = (9 + i) * depth + x
                buffer[at : at + 1, :] = ref[x, y : y + 1, :].astype(jnp.float32)
        for side, a, x in ((0, 1, depth - 1), (1, -1, 0)):
            for e in (-1, 0, 1):
                k = 9 * (a + 1) + 3 * (b + 1) + e + 1
                corner[side, e + 1 : e + 2, :] = collided[k, x, y : y + 1, :]
            for i, ref in enumerate(cell_refs):
                corner[side, 3 + i : 4 + i, :] = ref[x, y : y + 1, :].astype(jnp.float32)


def first_kernel(populations, kind, profile, rates, collided, *sends):
    depth, cells = populations.shape[1], populations.shape[3]

    def body(x, span):
        raw = along_axes([populations[k, x, :, span] for k in range(27)], to_moment)
        equal = equilibrium_terms(*density_velocity(raw))
        values = along_axes(relaxed(raw, equal, rates), from_moment)
        for k in range(27):
            collided[k, x, :, span] = values[k]

    tiles(depth, cells, body)
    pack(collided, sends, (kind, profile))


def shifted(plane, row, b, e, sublane):
    rows, cells = plane.shape
    if b:
        plane = pltpu.roll(plane, b % rows, 0)
        edge = 0 if b == 1 else rows - 1
        plane = jnp.where(sublane == edge, jnp.broadcast_to(row, plane.shape), plane)
    if e:
        plane = pltpu.roll(plane, e % cells, 1)
    return plane


def cell_fields(kind, profile, table):
    open_cell = (kind == 0) | (kind >= 3)
    vent = kind == 2
    velocity = vent_velocity(profile, table)
    return [jnp.where(open_cell, OPEN, 0.0)] + [jnp.where(vent, 6.0 * v, 0.0) for v in velocity]


def make_fields(halo, kind, profile, table, place, kinds_row, profiles_row, planes, edges):
    recv_x, recv_low, recv_high, corner_low, corner_high = halo
    depth = kind.shape[0]
    for x in range(-1, depth + 1):
        if 0 <= x < depth:
            kinds, profiles = kind[x].astype(jnp.float32), profile[x].astype(jnp.float32)
        else:
            side = 0 if x < 0 else 1
            kinds, profiles = recv_x[side, 9], recv_x[side, 10]
        for c, value in enumerate(cell_fields(kinds, profiles, table)):
            planes[c, x + 1] = value
    row_sides = ((recv_low, corner_low, 0), (recv_high, corner_high, PY - 1))
    for s, (buffer, corner, outer) in enumerate(row_sides):
        for target, i in ((kinds_row, 0), (profiles_row, 1)):
            target[...] = jnp.zeros(target.shape, jnp.float32)
            target[0:1, :] = corner[0, 3 + i : 4 + i, :]
            at = (9 + i) * depth
            for x in range(depth):
                target[x + 1 : x + 2, :] = buffer[at + x : at + x + 1, :]
            target[depth + 1 : depth + 2, :] = corner[1, 3 + i : 4 + i, :]
        kinds = jnp.where(place[0] == outer, 1.0, kinds_row[...])
        for c, value in enumerate(cell_fields(kinds, profiles_row[...], table)):
            edges[s, c] = value


def stream(collided, halo, bounce, passed, fields):
    recv_x, recv_low, recv_high, corner_low, corner_high = halo
    depth, rows, cells = collided.shape[1:]
    sublane = lax.broadcasted_iota(jnp.int32, (rows, cells), 0)
    lane = lax.broadcasted_iota(jnp.int32, (rows, cells), 1)
    for k in range(27):
        a, b, e = direction(k)
        for x in range(depth):
            if k == 13:
                passed[k, x] = collided[k, x]
                continue
            source = x - a
            side = 0 if source < 0 else 1
            inside = 0 <= source < depth
            plane = collided[k, source] if inside else recv_x[side, 3 * (b + 1) + e + 1]
            row = None
            if b:
                buffer, corner = (recv_low, corner_low) if b == 1 else (recv_high, corner_high)
                at = (3 * (a + 1) + e + 1) * depth + source
                row = buffer[at : at + 1, :] if inside else corner[side, e + 1 : e + 2, :]
            if fields is not None:
                planes, edges = fields

                def combine(read):
                    value = read(0)
                    for c, step in enumerate((a, b, e)):
                        if step:
                            value = value + read(c + 1) if step > 0 else value - read(c + 1)
                    return value

                term = combine(lambda c: planes[c, source + 1])
                term_row = None
                if b:
                    s = 0 if b == 1 else 1
                    term_row = combine(lambda c: edges[s, c, source + 1 : source + 2, :])
                term = shifted(term, term_row, b, e, sublane)
                if e:
                    term = jnp.where(lane == (0 if e == 1 else cells - 1), 0.0, term)
                bounce[k, x] = term
            term = bounce[k, x]
            value = shifted(plane, row, b, e, sublane)
            passed[k, x] = jnp.where(term > 0.5 * OPEN, value, collided[26 - k, x] + term)


def chosen(kind, profile, table, velocity):
    vent = vent_velocity(profile, table)
    return [
        jnp.where(kind == 3, vent[c], jnp.where(kind == 4, velocity[c], 0.0)) for c in range(3)
    ]


def collide_cells(passed, kind, profile, table, rates, collided):
    depth, cells = passed.shape[1], passed.shape[3]

    def body(x, span):
        kinds = kind[x, :, span]
        fluid = kinds == 0
        raw = along_axes([passed[k, x, :, span] for k in range(27)], to_moment)
        density, velocity = density_velocity(raw)
        forced = chosen(kinds, profile[x, :, span], table, velocity)
        density = jnp.where(fluid, density, 1.0)
        velocity = [jnp.where(fluid, velocity[c], forced[c]) for c in range(3)]
        equal = equilibrium_terms(density, velocity)
        mixed = relaxed(raw, equal, rates)
        values = [jnp.where(fluid, mixed[k], equal[k]) for k in range(27)]
        values = along_axes(values, from_moment)
        for k in range(27):
            collided[k, x, :, span] = values[k]

    tiles(depth, cells, body)


def finish_cells(passed, kind, profile, table, advanced):
    depth, cells = passed.shape[1], passed.shape[3]

    def body(x, span):
        kinds = kind[x, :, span]
        fluid = kinds == 0
        values = [passed[k, x, :, span] for k in range(27)]
        velocity = density_velocity(along_axes(values, to_moment))[1]
        ux, uy, uz = chosen(kinds, profile[x, :, span], table, velocity)
        base = 1.0 - 1.5 * (ux * ux + uy * uy + uz * uz)
        for k in range(27):
            projected = None
            for step, u in zip(direction(k), (ux, uy, uz)):
                if step:
                    signed = u if step > 0 else -u
                    projected = signed if projected is None else projected + signed
            equal = base if projected is None else base + projected * (3.0 + 4.5 * projected)
            advanced[k, x, :, span] = jnp.where(fluid, values[k], equal)

    tiles(depth, cells, body)


def second_kernel(*refs):
    collided, *halo = refs[:6]
    kind, profile, table, rates, place = refs[6:11]
    out, bounce = refs[11:13]
    sends = refs[13:18]
    passed, kinds_row, profiles_row, planes, edges = refs[18:]
    make_fields(halo, kind, profile, table, place, kinds_row, profiles_row, planes, edges)
    stream(collided, halo, bounce, passed, (planes, edges))
    collide_cells(passed, kind, profile, table, rates, out)
    pack(out, sends, ())


def middle_kernel(*refs):
    collided, *halo = refs[:6]
    bounce, kind, profile, table, rates = refs[6:11]
    out = refs[11]
    sends = refs[12:17]
    passed = refs[17]
    stream(collided, halo, bounce, passed, None)
    collide_cells(passed, kind, profile, table, rates, out)
    pack(out, sends, ())


def last_kernel(*refs):
    collided, *halo = refs[:6]
    bounce, kind, profile, table, advanced, passed = refs[6:]
    stream(collided, halo, bounce, passed, None)
    finish_cells(passed, kind, profile, table, advanced)


def passed_along(value, steps):
    count = lax.axis_size("gx")
    pairs = [(source, (source + steps) % count) for source in range(count)]
    return lax.ppermute(value, "gx", pairs)


def both_sides(value, across):
    if lax.axis_size("gx") == 2 * PY:
        return passed_along(value, PY + across)
    return jnp.stack(
        [passed_along(value[0], PY + across), passed_along(value[1], across - PY)]
    )


def resident(value):
    return pltpu.with_memory_space_constraint(value, pltpu.VMEM)


def exchange(sends):
    send_x, send_up, send_down, corner_up, corner_down = sends
    received = (
        both_sides(send_x, 0),
        passed_along(send_up, 1),
        passed_along(send_down, -1),
        both_sides(corner_up, 1),
        both_sides(corner_down, -1),
    )
    return tuple(pltpu.with_memory_space_constraint(h, pltpu.VMEM) for h in received)


def round_up(value, step):
    return -(-value // step) * step


def local(populations, cell_kind, profile, vent_table, rates):
    scaled = populations[:, 0]
    kind, profile = cell_kind[0], profile[0]
    depth, rows, cells = kind.shape
    f32 = jnp.float32
    field = jax.ShapeDtypeStruct(scaled.shape, f32)
    vmem = pl.BlockSpec(memory_space=pltpu.VMEM)
    smem = pl.BlockSpec(memory_space=pltpu.SMEM)
    place = ((lax.axis_index("gx") + PY // 2) % PY).astype(jnp.int32).reshape(1)

    def send_shapes(extra):
        along = jax.ShapeDtypeStruct((round_up((9 + extra) * depth, 8), cells), f32)
        corner = jax.ShapeDtypeStruct((2, 8, cells), f32)
        across = jax.ShapeDtypeStruct((2, 9 + extra, rows, cells), f32)
        return (across, along, along, corner, corner)

    def call(body, specs, outs, scratch, name):
        return pl.pallas_call(
            body,
            in_specs=specs,
            out_specs=jax.tree.map(lambda _: vmem, outs),
            out_shape=outs,
            scratch_shapes=scratch,
            name=name,
        )

    buffer = pltpu.VMEM(scaled.shape, f32)
    edge_rows = round_up(depth + 2, 8)
    collided, *sends = call(
        first_kernel, [vmem] * 3 + [smem], (field,) + send_shapes(2), [], "first"
    )(scaled, kind, profile, rates)
    collided = resident(collided)
    halo = exchange(sends)
    collided, bounce, *sends = call(
        second_kernel,
        [vmem] * 8 + [smem] * 3,
        (field, field) + send_shapes(0),
        [
            buffer,
            pltpu.VMEM((edge_rows, cells), f32),
            pltpu.VMEM((edge_rows, cells), f32),
            pltpu.VMEM((4, depth + 2, rows, cells), f32),
            pltpu.VMEM((2, 4, edge_rows, cells), f32),
        ],
        "second",
    )(collided, *halo, kind, profile, vent_table, rates, place)
    bounce = resident(bounce)
    for _ in range(STEPS - 2):
        collided = resident(collided)
        halo = exchange(sends)
        collided, *sends = call(
            middle_kernel,
            [vmem] * 9 + [smem] * 2,
            (field,) + send_shapes(0),
            [buffer],
            "middle",
        )(collided, *halo, bounce, kind, profile, vent_table, rates)
    collided = resident(collided)
    halo = exchange(sends)
    advanced = call(last_kernel, [vmem] * 9 + [smem], field, [buffer], "last")(
        collided, *halo, bounce, kind, profile, vent_table
    )
    return advanced[:, None]


def solution(mesh):
    return jax.shard_map(
        local,
        mesh=mesh,
        in_specs=(
            P("scen", "gx", None, None, None),
            P("gx", None, None, "scen"),
            P("gx", None, None, "scen"),
            P("scen", None),
            P(),
        ),
        out_specs=P("scen", "gx", None, None, None),
        check_vma=False,
    )
```
